128 devices in a mesh: date: 16 (over y, x), pix: 4 (over z), tile: 2 (over core).
Axes of the slice: x: 4, y: 4, z: 4, core: 2. Of those that a mesh axis runs over, the one named last changes fastest.
Arguments:
- reflectance: float32 [128, 7, 65536], P('date', None, ('tile', 'pix')), parts along dimension 2, may hold values from -6 to 6
- validity: int32 [128, 65536], P('date', ('tile', 'pix')), parts along dimension 1, may hold values from 0 to 1, as said below
- day_number: int32 [128], P('date'), may hold values from 1 to 255, as said below
Outputs:
- filled: float32 [128, 7, 65536], P('date', None, ('tile', 'pix')), parts along dimension 2
The draws below stay inside these ranges and needn't reach their ends.
There are 2 independent parts, one for each index of `tile`. The reference program is written for one: setup_inputs(seed, part) draws one part's arguments, and reference() takes and returns one part's arrays. A program takes and returns all parts, laid end to end along the dimension named above; an argument that names none is the same for every part. Nothing has to cross between parts.
Inputs may be any that keep to these rules, and one draw needn't show every extreme that they name: `validity`: 1 marks a usable observation, 0 a rejected one. `day_number`: strictly increasing along the dates, by 1 to 3 days from one date to the next, starting at day 1.
All inputs are finite; a program needn't handle non-finite values.
Results may differ from the reference program's by a relative error of at most 0.0003.
Values sent between devices are 32-bit elements; how exact they have to be, the bound alone decides.
A program may use at most 64 MiB of HBM per device.

```python
import jax
import jax.numpy as jnp
from jax import lax

BANDS = 7
DATE_DEV = 8
DATES = 128
PIXELS = 32768


def draw_validity(key, part):
    picks = jax.random.randint(jax.random.fold_in(key, 11), (DATES, PIXELS), 0, 2 * DATE_DEV)
    kinds = jax.random.randint(jax.random.fold_in(key, 13), (PIXELS,), 0, 64)
    early = jax.random.randint(jax.random.fold_in(key, 17), (PIXELS,), 0, DATE_DEV)
    late = DATES - 1 - jax.random.randint(jax.random.fold_in(key, 19), (PIXELS,), 0, DATE_DEV)
    lonely = jax.random.randint(jax.random.fold_in(key, 29), (PIXELS,), 0, DATES)
    rows = lax.broadcasted_iota(jnp.int32, (DATES, PIXELS), 0)
    common = picks < 2
    at_ends = (rows == early[None, :]) | (rows == late[None, :])
    single = rows == lonely[None, :]
    kind_row = kinds[None, :]
    live = jnp.where(kind_row == 0, False, jnp.where(kind_row <= 2, at_ends, jnp.where(kind_row == 3, single, common)))
    return live.astype(jnp.int32)


def draw_day_number(key, part):
    picks = jax.random.randint(jax.random.fold_in(key, 23), (DATES,), 1, 4).astype(jnp.int32)
    before = jnp.roll(picks, 1)
    order = lax.broadcasted_iota(jnp.int32, (DATES,), 0)
    odd_step = jnp.where(order == DATES - 1, 2, picks)
    steps = jnp.where(order == 0, 1, jnp.where(order % 2 == 1, odd_step, 4 - before))
    return jnp.cumsum(steps).astype(jnp.int32)


def block_scale(own_key, extent, cuts, least, top_value):
    gain = 1.0
    for dim, parts in cuts:
        steps = jax.random.uniform(jax.random.fold_in(jax.random.fold_in(own_key, 6), dim), (parts,), jnp.float32, least / len(cuts), top_value / len(cuts))
        gain = gain * jnp.repeat(jnp.exp(steps), extent[dim] // parts).reshape((-1,) + (1,) * (len(extent) - 1 - dim))
    return gain


def scatter_about(own_key, dims, scale, bound, shards=(), dtype=jnp.bfloat16):
    array = scale * jax.random.normal(own_key, dims, jnp.float32)
    if shards:
        array = array * block_scale(own_key, dims, shards, -0.22, 0.18)
    return jnp.clip(array, -bound, bound).astype(dtype)


def setup_inputs(seed: int = 0, part: int = 0) -> dict:
    arg_keys = jax.random.split(jax.random.key(seed), 4)
    part_keys = jax.random.split(jax.random.fold_in(arg_keys[3], part), 4)
    return {
        "reflectance": scatter_about(part_keys[0], (DATES, BANDS, PIXELS), 1.0, 6.0, ((0, 16), (2, 4)), jnp.float32),
        "validity": draw_validity(jax.random.fold_in(jax.random.fold_in(arg_keys[3], part), 71), part),
        "day_number": draw_day_number(jax.random.fold_in(arg_keys[3], 71), part),
    }


far_day = 1073741824


def scan_block(values, validity, days):
    count = values.shape[0]
    live = validity > 0
    order = lax.broadcasted_iota(jnp.int32, validity.shape, 0)
    fwd_pos = lax.cummax(jnp.where(live, order, -1), axis=0)
    bwd_pos = lax.cummin(jnp.where(live, order, count), axis=0, reverse=True)
    fwd_val = jnp.take_along_axis(values, jnp.clip(fwd_pos, 0, count - 1)[:, None, :], axis=0)
    bwd_val = jnp.take_along_axis(values, jnp.clip(bwd_pos, 0, count - 1)[:, None, :], axis=0)
    day_col = jnp.broadcast_to(days[:, None], validity.shape).astype(jnp.int32)
    fwd_day = lax.cummax(jnp.where(live, day_col, -1), axis=0)
    bwd_day = lax.cummin(jnp.where(live, day_col, far_day), axis=0, reverse=True)
    return live, day_col, fwd_day, fwd_val, bwd_day, bwd_val


def blend(values, live, day_col, fwd_day, fwd_val, bwd_day, bwd_val):
    has_prev = fwd_day >= 0
    has_next = bwd_day < far_day
    inside = has_prev & has_next & jnp.logical_not(live)
    span = jnp.where(inside, bwd_day - fwd_day, 1).astype(jnp.float32)
    weight = (day_col - fwd_day).astype(jnp.float32) / span
    middle = fwd_val + weight[:, None, :] * (bwd_val - fwd_val)
    one_side = jnp.where(has_prev[:, None, :], fwd_val,
                         jnp.where(has_next[:, None, :], bwd_val, jnp.zeros_like(fwd_val)))
    chosen = jnp.where(inside[:, None, :], middle, one_side)
    return jnp.where(live[:, None, :], values, chosen)


def reference(reflectance, validity, day_number):
    live, day_col, fwd_day, fwd_val, bwd_day, bwd_val = scan_block(reflectance, validity, day_number)
    return blend(reflectance, live, day_col, fwd_day, fwd_val, bwd_day, bwd_val)
```

```python
import functools

import jax
import jax.numpy as jnp
from jax import lax
from jax.experimental import pallas as pl
from jax.experimental.pallas import tpu as pltpu
from jax.sharding import Mesh
from jax.sharding import PartitionSpec as P

MESH = pl.DeviceIdType.MESH
DATE = ("date_0", "date_1")
LANES = 128
ROWS = 8
TILES = 4
STAGES = 4
LAG = 3
NONE = -1073741824.0


def spread(row):
    return jnp.broadcast_to(row, (ROWS, LANES))


def scan_fill(
    bands,
    chunks,
    days_hbm,
    x_hbm,
    v_hbm,
    out_ref,
    days,
    xv,
    vv,
    own,
    come,
    enter,
    day_sem,
    x_sem,
    v_sem,
    send_sem,
    recv_sem,
):
    width = TILES * LANES
    yi = lax.axis_index(DATE[0])
    xi = lax.axis_index(DATE[1])
    partner = (
        {DATE[1]: xi + 1 - 2 * lax.rem(xi, 2)},
        {DATE[1]: 3 - xi},
        {DATE[0]: yi + 1 - 2 * lax.rem(yi, 2)},
        {DATE[0]: 3 - yi},
    )
    upper = (lax.rem(xi, 2), xi // 2, lax.rem(yi, 2), yi // 2)

    def load_x(c):
        cols = pl.ds(pl.multiple_of(c * width, width), width)
        return pltpu.make_async_copy(x_hbm.at[:, :, cols], xv.at[:, :, cols], x_sem.at[c])

    def load_v(c):
        cols = pl.ds(pl.multiple_of(c * width, width), width)
        return pltpu.make_async_copy(v_hbm.at[:, cols], vv.at[:, cols], v_sem.at[c])

    def exchange(stage, c):
        return pltpu.make_async_remote_copy(
            src_ref=own.at[stage, c],
            dst_ref=come.at[stage, c],
            send_sem=send_sem.at[stage, c],
            recv_sem=recv_sem.at[stage, c],
            device_id=partner[stage],
            device_id_type=MESH,
        )

    day_copy = pltpu.make_async_copy(days_hbm, days, day_sem)
    day_copy.start()

    @pl.loop(0, chunks)
    def _(c):
        load_v(c).start()
        load_x(c).start()

    barrier = pltpu.get_barrier_semaphore()
    for who in partner:
        pl.semaphore_signal(barrier, inc=1, device_id=who, device_id_type=MESH)

    day_copy.wait()
    sub = lax.broadcasted_iota(jnp.int32, (ROWS, LANES), 0)
    day_col = jnp.zeros((ROWS, LANES), jnp.float32)
    for t in range(ROWS):
        day_col = jnp.where(sub == t, days[t].astype(jnp.float32), day_col)
    lower_rows = sub < TILES
    pl.semaphore_wait(barrier, len(partner))

    def summarize(c):
        load_v(c).wait()
        load_x(c).wait()
        for j in range(TILES):
            cols = pl.ds(pl.multiple_of(c * width + j * LANES, LANES), LANES)
            live = vv[:, cols] > 0
            last = jnp.max(jnp.where(live, day_col, NONE), axis=0, keepdims=True)
            first = jnp.max(jnp.where(live, -day_col, NONE), axis=0, keepdims=True)
            own[0, c, bands, pl.ds(j, 1), :] = last
            own[0, c, bands, pl.ds(TILES + j, 1), :] = first
            at_last = day_col == spread(last)
            at_first = -day_col == spread(first)
            for b in range(bands):
                x = xv[b, :, cols]
                own[0, c, b, pl.ds(j, 1), :] = jnp.sum(
                    jnp.where(at_last, x, 0.0), axis=0, keepdims=True
                )
                own[0, c, b, pl.ds(TILES + j, 1), :] = jnp.sum(
                    jnp.where(at_first, x, 0.0), axis=0, keepdims=True
                )
        exchange(0, c).start()

    def merge(stage, c):
        exchange(stage, c).wait_recv()
        near = lower_rows == (jnp.full((ROWS, LANES), upper[stage], jnp.int32) > 0)
        key = own[stage, c, bands]
        other = come[stage, c, bands]
        if stage + 1 < STAGES:
            take = other > key
            for b in range(bands + 1):
                own[stage + 1, c, b] = jnp.where(take, come[stage, c, b], own[stage, c, b])
            exchange(stage + 1, c).start()
        if stage == 0:
            take = near & (other > NONE)
            for b in range(bands):
                enter[c, b] = jnp.where(take, come[stage, c, b], 0.0)
            enter[c, bands] = jnp.where(take, other, NONE)
        else:
            take = near & (other > enter[c, bands])
            for b in range(bands + 1):
                enter[c, b] = jnp.where(take, come[stage, c, b], enter[c, b])

    def complete(c):
        e_key = enter[c, bands]
        o_key = own[0, c, bands]
        e_has = e_key > NONE
        o_has = o_key > NONE
        flip = functools.partial(pltpu.roll, shift=TILES, axis=0)
        for b in range(bands):
            e = enter[c, b]
            enter[c, b] = jnp.where(e_has, e, flip(jnp.where(o_has, own[0, c, b], e)))
        e_day = jnp.where(lower_rows, e_key, -e_key)
        o_day = jnp.where(lower_rows, o_key, -o_key)
        enter[c, bands] = jnp.where(e_has, e_day, flip(jnp.where(o_has, o_day, e_day)))
        for j in range(TILES):
            cols = pl.ds(pl.multiple_of(c * width + j * LANES, LANES), LANES)
            live = vv[:, cols] > 0
            before = jnp.where(live, sub, -1)
            after = jnp.where(live, sub, ROWS)
            for k in (1, 2, 4):
                before = jnp.maximum(
                    before, jnp.where(sub >= k, pltpu.roll(before, k, axis=0), -1)
                )
                after = jnp.minimum(
                    after, jnp.where(sub < ROWS - k, pltpu.roll(after, ROWS - k, axis=0), ROWS)
                )
            has_f = before >= 0
            has_b = after < ROWS
            at_f = jnp.maximum(before, 0)
            at_b = jnp.minimum(after, ROWS - 1)

            def sides(x, b):
                f = jnp.take_along_axis(x, at_f, axis=0)
                n = jnp.take_along_axis(x, at_b, axis=0)
                f = jnp.where(has_f, f, spread(enter[c, b, pl.ds(j, 1), :]))
                n = jnp.where(has_b, n, spread(enter[c, b, pl.ds(TILES + j, 1), :]))
                return f, n

            prev, following = sides(day_col, bands)
            span = following - prev
            weight = (day_col - prev) / jnp.where(span == 0.0, 1.0, span)
            for b in range(bands):
                f, n = sides(xv[b, :, cols], b)
                out_ref[b, :, cols] = f + weight * (n - f)

    @pl.loop(0, chunks)
    def _(c):
        summarize(c)

    @pl.loop(0, chunks + LAG * (STAGES - 1))
    def _(t):
        for stage in range(STAGES):
            c = t - LAG * stage

            @pl.when((c >= 0) & (c < chunks))
            def _():
                merge(stage, c)
                if stage == STAGES - 1:
                    complete(c)

    @pl.loop(0, chunks)
    def _(c):
        for stage in range(STAGES):
            exchange(stage, c).wait_send()


def body(reflectance, validity, day_number):
    dates, bands, pixels = reflectance.shape
    chunks = pixels // (TILES * LANES)
    hbm = pl.BlockSpec(memory_space=pltpu.HBM)
    filled = pl.pallas_call(
        functools.partial(scan_fill, bands, chunks),
        out_shape=pltpu.VMEM((bands, dates, pixels), jnp.float32),
        in_specs=[hbm, hbm, hbm],
        out_specs=pl.BlockSpec(memory_space=pltpu.VMEM),
        scratch_shapes=[
            pltpu.SMEM((dates,), jnp.int32),
            pltpu.VMEM((bands, dates, pixels), jnp.float32),
            pltpu.VMEM((dates, pixels), jnp.int32),
            pltpu.VMEM((STAGES, chunks, bands + 1, ROWS, LANES), jnp.float32),
            pltpu.VMEM((STAGES, chunks, bands + 1, ROWS, LANES), jnp.float32),
            pltpu.VMEM((chunks, bands + 1, ROWS, LANES), jnp.float32),
            pltpu.SemaphoreType.DMA,
            pltpu.SemaphoreType.DMA((chunks,)),
            pltpu.SemaphoreType.DMA((chunks,)),
            pltpu.SemaphoreType.DMA((STAGES, chunks)),
            pltpu.SemaphoreType.DMA((STAGES, chunks)),
        ],
        compiler_params=pltpu.CompilerParams(
            collective_id=0, has_side_effects=True, vmem_limit_bytes=(62 << 20) - 65536
        ),
        name="scan_fill",
    )(day_number, jnp.transpose(reflectance, (1, 0, 2)), validity)
    return jnp.transpose(filled, (1, 0, 2))


def solution(mesh):
    torus = Mesh(
        mesh.devices.reshape(4, 4, mesh.shape["pix"], mesh.shape["tile"]),
        ("date_0", "date_1", "pix", "tile"),
    )
    placed = (P(DATE, None, ("tile", "pix")), P(DATE, ("tile", "pix")), P(DATE))
    return jax.shard_map(
        body, mesh=torus, in_specs=placed, out_specs=P(DATE, None, ("tile", "pix")), check_vma=False
    )
```

```python
import functools

import jax
import jax.numpy as jnp
from jax import lax
from jax.experimental import pallas as pl
from jax.experimental.pallas import tpu as pltpu
from jax.sharding import Mesh
from jax.sharding import PartitionSpec as P

MESH = pl.DeviceIdType.MESH
DATE = ("date_0", "date_1")
LANES = 128
ROWS = 8
TILES = 4
SIDE = 4
NONE = -1073741824.0
SHARES = (1, 1, 2, 2, 2, 2, 2, 2, 1, 1)
LOADS = (1, 1, 2, 4, 8)
STEP, HOP, FAR = 0.7, 2.4, 3.2


def spans(shares, groups):
    scale = groups // sum(shares) if groups >= sum(shares) else 0
    if scale == 0:
        return [(g, 1) for g in range(groups)]
    starts, at = [], 0
    for share in shares:
        starts.append((at, share * scale))
        at += share * scale
    return starts


def arrival_order(messages):
    events, ready = [], [0.0] * len(messages)
    for stage, delay in enumerate((HOP, HOP, FAR)):
        link = 0.0
        for m, (_, count) in enumerate(messages):
            link = max(link, ready[m]) + STEP * count
            ready[m] = link + delay
            events.append((ready[m], stage, m))
    return [(stage, m) for _, stage, m in sorted(events)]


def scan_fill(
    bands,
    groups,
    days_hbm,
    x_hbm,
    v_hbm,
    out_ref,
    days,
    xv,
    vv,
    own,
    come,
    come_y,
    enter,
    day_sem,
    x_sem,
    v_sem,
    send_sem,
    recv_sem,
):
    width = TILES * LANES
    packs = (bands + 1) // 2
    messages, loads = spans(SHARES, groups), spans(LOADS, groups)
    yi = lax.axis_index(DATE[0])
    xi = lax.axis_index(DATE[1])
    pair = ({DATE[1]: xi + 1 - 2 * lax.rem(xi, 2)}, {DATE[1]: 3 - xi})
    taken = (1 - lax.rem(xi, 2), 1 - xi // 2)
    rows = [{DATE[0]: lax.rem(yi + d, SIDE)} for d in range(1, SIDE)]
    row_gives = [(yi + d) // SIDE for d in range(1, SIDE)]
    row_takes = [1 - (yi + SIDE - d) // SIDE for d in range(1, SIDE)]

    def load_x(i):
        cols = pl.ds(loads[i][0] * width, loads[i][1] * width)
        return pltpu.make_async_copy(x_hbm.at[:, :, cols], xv.at[:, :, cols], x_sem.at[i])

    def load_v(i):
        cols = pl.ds(loads[i][0] * width, loads[i][1] * width)
        return pltpu.make_async_copy(v_hbm.at[:, cols], vv.at[:, cols], v_sem.at[i])

    def swap(stage, m):
        part = pl.ds(*messages[m])
        return pltpu.make_async_remote_copy(
            src_ref=own.at[stage, part],
            dst_ref=come.at[stage, part],
            send_sem=send_sem.at[stage],
            recv_sem=recv_sem.at[stage, m],
            device_id=pair[stage],
            device_id_type=MESH,
        )

    def to_row(d, m):
        part = pl.ds(*messages[m])
        return pltpu.make_async_remote_copy(
            src_ref=own.at[2, part, row_gives[d]],
            dst_ref=come_y.at[part, d],
            send_sem=send_sem.at[2],
            recv_sem=recv_sem.at[2, m],
            device_id=rows[d],
            device_id_type=MESH,
        )

    def from_rows(part, m):
        return pltpu.make_async_remote_copy(
            src_ref=come_y.at[part],
            dst_ref=come_y.at[part],
            send_sem=send_sem.at[2],
            recv_sem=recv_sem.at[2, m],
            device_id=rows[0],
            device_id_type=MESH,
        )

    barrier = pltpu.get_barrier_semaphore()
    for who in (*pair, *rows):
        pl.semaphore_signal(barrier, inc=1, device_id=who, device_id_type=MESH)
    day_copy = pltpu.make_async_copy(days_hbm, days, day_sem)
    day_copy.start()
    for i in range(len(loads)):
        load_v(i).start()
        load_x(i).start()

    day_copy.wait()
    sub = lax.broadcasted_iota(jnp.int32, (ROWS, LANES), 0)
    day_col = jnp.zeros((ROWS, LANES), jnp.float32)
    for t in range(ROWS):
        day_col = jnp.where(sub == t, days[t].astype(jnp.float32), day_col)
    key_rows = sub >= TILES

    def lanes_of(g, j):
        return pl.ds(pl.multiple_of(g * width + j * LANES, LANES), LANES)

    def key_of(pack):
        return jnp.where(key_rows, pack, pltpu.roll(pack, TILES, axis=0))

    def spread(row):
        return jnp.broadcast_to(row, (ROWS, LANES))

    def row_of(band, j):
        return band // 2, pl.ds((band % 2) * TILES + j, 1)

    def over(m, work):
        start, count = messages[m]
        if count == 1:
            work(start)
        else:
            pl.loop(start, start + count)(work)

    def summarize(g):
        for j in range(TILES):
            cols = lanes_of(g, j)
            live = vv[:, cols] > 0
            last = jnp.max(jnp.where(live, day_col, NONE), axis=0, keepdims=True)
            first = jnp.max(jnp.where(live, -day_col, NONE), axis=0, keepdims=True)
            at_last = day_col == spread(last)
            at_first = -day_col == spread(first)
            for b in range(bands):
                x = xv[b, :, cols]
                p, r = row_of(b, j)
                own[0, g, 0, p, r, :] = jnp.sum(jnp.where(at_last, x, 0.0), axis=0, keepdims=True)
                own[0, g, 1, p, r, :] = jnp.sum(jnp.where(at_first, x, 0.0), axis=0, keepdims=True)
            p, r = row_of(bands, j)
            own[0, g, 0, p, r, :] = last
            own[0, g, 1, p, r, :] = first

    def merge_pair(stage, g):
        for side in range(2):
            take = key_of(come[stage, g, side, packs - 1]) > key_of(own[stage, g, side, packs - 1])
            for p in range(packs):
                own[stage + 1, g, side, p] = jnp.where(
                    take, come[stage, g, side, p], own[stage, g, side, p]
                )

    def note_pair(stage, g):
        side = taken[stage]
        if stage == 0:
            for p in range(packs):
                enter[g, side, p] = come[0, g, side, p]
                enter[g, 1 - side, p] = jnp.where(key_rows, NONE if p == packs - 1 else 0.0, 0.0)
        else:
            take = key_of(come[stage, g, side, packs - 1]) > key_of(enter[g, side, packs - 1])
            for p in range(packs):
                enter[g, side, p] = jnp.where(take, come[stage, g, side, p], enter[g, side, p])

    def complete(g):
        for d in range(SIDE - 1):
            side = row_takes[d]
            take = key_of(come_y[g, d, packs - 1]) > key_of(enter[g, side, packs - 1])
            for p in range(packs):
                enter[g, side, p] = jnp.where(take, come_y[g, d, p], enter[g, side, p])
        has = [key_of(enter[g, s, packs - 1]) > NONE for s in range(2)]
        mine = [key_of(own[0, g, s, packs - 1]) > NONE for s in range(2)]
        for p in range(packs):
            ends = [enter[g, s, p] for s in range(2)]
            other = [jnp.where(mine[s], own[0, g, s, p], ends[s]) for s in range(2)]
            if p == packs - 1:
                other = [jnp.where(key_rows, -o, o) for o in other]
            for s in range(2):
                enter[g, s, p] = jnp.where(has[s], ends[s], other[1 - s])
        for j in range(TILES):
            cols = lanes_of(g, j)
            live = vv[:, cols] > 0
            before = jnp.where(live, sub, -1)
            after = jnp.where(live, sub, ROWS)
            for k in (1, 2, 4):
                before = jnp.maximum(
                    before, jnp.where(sub >= k, pltpu.roll(before, k, axis=0), -1)
                )
                after = jnp.minimum(
                    after, jnp.where(sub < ROWS - k, pltpu.roll(after, ROWS - k, axis=0), ROWS)
                )
            has_f = before >= 0
            has_b = after < ROWS
            at_f = jnp.maximum(before, 0)
            at_b = jnp.minimum(after, ROWS - 1)

            def sides(x, b, sign):
                p, r = row_of(b, j)
                f = jnp.take_along_axis(x, at_f, axis=0)
                n = jnp.take_along_axis(x, at_b, axis=0)
                f = jnp.where(has_f, f, spread(enter[g, 0, p, r, :]))
                n = jnp.where(has_b, n, spread(sign * enter[g, 1, p, r, :]))
                return f, n

            prev, following = sides(day_col, bands, -1.0)
            span = following - prev
            weight = (day_col - prev) / jnp.where(span == 0.0, 1.0, span)
            for b in range(bands):
                f, n = sides(xv[b, :, cols], b, 1.0)
                out_ref[b, :, cols] = f + weight * (n - f)

    loaded = 0
    for m, (start, count) in enumerate(messages):
        while loaded < len(loads) and loads[loaded][0] < start + count:
            load_v(loaded).wait()
            load_x(loaded).wait()
            loaded += 1
        over(m, summarize)
        if m == 0:
            pl.semaphore_wait(barrier, len(pair) + len(rows))
        swap(0, m).start()

    for stage, m in arrival_order(messages):
        if stage < 2:
            swap(stage, m).wait_recv()
            over(m, functools.partial(merge_pair, stage))
            if stage == 0:
                swap(1, m).start()
            else:
                for d in range(SIDE - 1):
                    to_row(d, m).start()
            over(m, functools.partial(note_pair, stage))
        else:
            from_rows(pl.ds(*messages[m]), m).wait_recv()
            over(m, complete)

    for stage in range(2):
        pltpu.make_async_remote_copy(
            src_ref=own.at[stage],
            dst_ref=come.at[stage],
            send_sem=send_sem.at[stage],
            recv_sem=recv_sem.at[stage, 0],
            device_id=pair[stage],
            device_id_type=MESH,
        ).wait_send()
    from_rows(pl.ds(0, groups), 0).wait_send()


def body(reflectance, validity, day_number):
    dates, bands, pixels = reflectance.shape
    groups = pixels // (TILES * LANES)
    packs = (bands + 1) // 2
    messages, loads = len(spans(SHARES, groups)), len(spans(LOADS, groups))
    hbm = pl.BlockSpec(memory_space=pltpu.HBM)
    filled = pl.pallas_call(
        functools.partial(scan_fill, bands, groups),
        out_shape=pltpu.VMEM((bands, dates, pixels), jnp.float32),
        in_specs=[hbm, hbm, hbm],
        out_specs=pl.BlockSpec(memory_space=pltpu.VMEM),
        scratch_shapes=[
            pltpu.SMEM((dates,), jnp.int32),
            pltpu.VMEM((bands, dates, pixels), jnp.float32),
            pltpu.VMEM((dates, pixels), jnp.int32),
            pltpu.VMEM((3, groups, 2, packs, ROWS, LANES), jnp.float32),
            pltpu.VMEM((2, groups, 2, packs, ROWS, LANES), jnp.float32),
            pltpu.VMEM((groups, SIDE - 1, packs, ROWS, LANES), jnp.float32),
            pltpu.VMEM((groups, 2, packs, ROWS, LANES), jnp.float32),
            pltpu.SemaphoreType.DMA,
            pltpu.SemaphoreType.DMA((loads,)),
            pltpu.SemaphoreType.DMA((loads,)),
            pltpu.SemaphoreType.DMA((3,)),
            pltpu.SemaphoreType.DMA((3, messages)),
        ],
        compiler_params=pltpu.CompilerParams(
            collective_id=0, has_side_effects=True, vmem_limit_bytes=(62 << 20) - 65536
        ),
        name="scan_fill",
    )(day_number, jnp.transpose(reflectance, (1, 0, 2)), validity)
    return jnp.transpose(filled, (1, 0, 2))


def solution(mesh):
    torus = Mesh(
        mesh.devices.reshape(4, 4, mesh.shape["pix"], mesh.shape["tile"]),
        ("date_0", "date_1", "pix", "tile"),
    )
    placed = (P(DATE, None, ("tile", "pix")), P(DATE, ("tile", "pix")), P(DATE))
    return jax.shard_map(
        body, mesh=torus, in_specs=placed, out_specs=P(DATE, None, ("tile", "pix")), check_vma=False
    )
```

```python
import functools

import jax
import jax.numpy as jnp
from jax import lax
from jax.experimental import pallas as pl
from jax.experimental.pallas import tpu as pltpu
from jax.sharding import Mesh
from jax.sharding import PartitionSpec as P

MESH = pl.DeviceIdType.MESH
DATE = ("date_0", "date_1")
LANES = 128
ROWS = 8
TILES = 4
SIDE = 4
NONE = -1073741824.0
SHARES = (1, 1, 2, 2, 2, 2, 2, 2, 1, 1)
LOADS = (2, 6, 8)
STEP, HOP, FAR = 0.7, 3.0, 3.8


def spans(shares, groups):
    scale = groups // sum(shares) if groups >= sum(shares) else 0
    if scale == 0:
        return [(g, 1) for g in range(groups)]
    starts, at = [], 0
    for share in shares:
        starts.append((at, share * scale))
        at += share * scale
    return starts


def arrival_order(messages):
    events, ready = [], [0.0] * len(messages)
    for stage, delay in enumerate((HOP, HOP, FAR)):
        link = 0.0
        for m, (_, count) in enumerate(messages):
            link = max(link, ready[m]) + STEP * count
            ready[m] = link + delay
            events.append((ready[m], stage, m))
    return [(stage, m) for _, stage, m in sorted(events)]


def scan_fill(
    bands,
    groups,
    days_hbm,
    x_hbm,
    v_hbm,
    out_ref,
    days,
    xv,
    vv,
    own,
    come,
    come_y,
    enter,
    day_sem,
    x_sem,
    v_sem,
    send_sem,
    recv_sem,
):
    width = TILES * LANES
    packs = (bands + 1) // 2
    messages, loads = spans(SHARES, groups), spans(LOADS, groups)
    yi = lax.axis_index(DATE[0])
    xi = lax.axis_index(DATE[1])
    pair = ({DATE[1]: xi + 1 - 2 * lax.rem(xi, 2)}, {DATE[1]: 3 - xi})
    taken = (1 - lax.rem(xi, 2), 1 - xi // 2)
    rows = [{DATE[0]: lax.rem(yi + d, SIDE)} for d in range(1, SIDE)]
    row_gives = [(yi + d) // SIDE for d in range(1, SIDE)]
    row_takes = [1 - (yi + SIDE - d) // SIDE for d in range(1, SIDE)]

    def load_x(i):
        cols = pl.ds(loads[i][0] * width, loads[i][1] * width)
        return pltpu.make_async_copy(x_hbm.at[:, :, cols], xv.at[:, :, cols], x_sem.at[i])

    def load_v(i):
        cols = pl.ds(loads[i][0] * width, loads[i][1] * width)
        return pltpu.make_async_copy(v_hbm.at[:, cols], vv.at[:, cols], v_sem.at[i])

    def swap(stage, m):
        part = pl.ds(*messages[m])
        return pltpu.make_async_remote_copy(
            src_ref=own.at[stage, part],
            dst_ref=come.at[stage, part],
            send_sem=send_sem.at[stage],
            recv_sem=recv_sem.at[stage, m],
            device_id=pair[stage],
            device_id_type=MESH,
        )

    def to_row(d, m):
        part = pl.ds(*messages[m])
        return pltpu.make_async_remote_copy(
            src_ref=own.at[2, part, row_gives[d]],
            dst_ref=come_y.at[part, d],
            send_sem=send_sem.at[2],
            recv_sem=recv_sem.at[2, m],
            device_id=rows[d],
            device_id_type=MESH,
        )

    def from_rows(part, m):
        return pltpu.make_async_remote_copy(
            src_ref=come_y.at[part],
            dst_ref=come_y.at[part],
            send_sem=send_sem.at[2],
            recv_sem=recv_sem.at[2, m],
            device_id=rows[0],
            device_id_type=MESH,
        )

    barrier = pltpu.get_barrier_semaphore()
    for who in (*pair, *rows):
        pl.semaphore_signal(barrier, inc=1, device_id=who, device_id_type=MESH)
    day_copy = pltpu.make_async_copy(days_hbm, days, day_sem)
    day_copy.start()
    for i in range(len(loads)):
        load_v(i).start()
        load_x(i).start()

    day_copy.wait()
    sub = lax.broadcasted_iota(jnp.int32, (ROWS, LANES), 0)
    day_col = jnp.zeros((ROWS, LANES), jnp.float32)
    for t in range(ROWS):
        day_col = jnp.where(sub == t, days[t].astype(jnp.float32), day_col)
    key_rows = sub >= TILES

    def lanes_of(g, j):
        return pl.ds(pl.multiple_of(g * width + j * LANES, LANES), LANES)

    def key_of(pack):
        return jnp.where(key_rows, pack, pltpu.roll(pack, TILES, axis=0))

    def spread(row):
        return jnp.broadcast_to(row, (ROWS, LANES))

    def row_of(band, j):
        return band // 2, pl.ds((band % 2) * TILES + j, 1)

    def over(m, work):
        start, count = messages[m]
        if count == 1:
            work(start)
        else:
            pl.loop(start, start + count)(work)

    def summarize(g):
        for j in range(TILES):
            cols = lanes_of(g, j)
            live = vv[:, cols] > 0
            last = jnp.max(jnp.where(live, day_col, NONE), axis=0, keepdims=True)
            first = jnp.max(jnp.where(live, -day_col, NONE), axis=0, keepdims=True)
            at_last = day_col == spread(last)
            at_first = -day_col == spread(first)
            for b in range(bands):
                x = xv[b, :, cols]
                p, r = row_of(b, j)
                own[0, g, 0, p, r, :] = jnp.sum(jnp.where(at_last, x, 0.0), axis=0, keepdims=True)
                own[0, g, 1, p, r, :] = jnp.sum(jnp.where(at_first, x, 0.0), axis=0, keepdims=True)
            p, r = row_of(bands, j)
            own[0, g, 0, p, r, :] = last
            own[0, g, 1, p, r, :] = first

    def merge_pair(stage, g):
        for side in range(2):
            take = key_of(come[stage, g, side, packs - 1]) > key_of(own[stage, g, side, packs - 1])
            for p in range(packs):
                own[stage + 1, g, side, p] = jnp.where(
                    take, come[stage, g, side, p], own[stage, g, side, p]
                )

    def note_pair(stage, g):
        side = taken[stage]
        if stage == 0:
            for p in range(packs):
                enter[g, side, p] = come[0, g, side, p]
                enter[g, 1 - side, p] = jnp.where(key_rows, NONE if p == packs - 1 else 0.0, 0.0)
        else:
            take = key_of(come[stage, g, side, packs - 1]) > key_of(enter[g, side, packs - 1])
            for p in range(packs):
                enter[g, side, p] = jnp.where(take, come[stage, g, side, p], enter[g, side, p])

    def complete(g):
        for d in range(SIDE - 1):
            side = row_takes[d]
            take = key_of(come_y[g, d, packs - 1]) > key_of(enter[g, side, packs - 1])
            for p in range(packs):
                enter[g, side, p] = jnp.where(take, come_y[g, d, p], enter[g, side, p])
        has = [key_of(enter[g, s, packs - 1]) > NONE for s in range(2)]
        mine = [key_of(own[0, g, s, packs - 1]) > NONE for s in range(2)]
        for p in range(packs):
            ends = [enter[g, s, p] for s in range(2)]
            other = [jnp.where(mine[s], own[0, g, s, p], ends[s]) for s in range(2)]
            if p == packs - 1:
                other = [jnp.where(key_rows, -o, o) for o in other]
            for s in range(2):
                enter[g, s, p] = jnp.where(has[s], ends[s], other[1 - s])
        for j in range(TILES):
            cols = lanes_of(g, j)
            live = vv[:, cols] > 0
            before = jnp.where(live, sub, -1)
            after = jnp.where(live, sub, ROWS)
            for k in (1, 2, 4):
                before = jnp.maximum(
                    before, jnp.where(sub >= k, pltpu.roll(before, k, axis=0), -1)
                )
                after = jnp.minimum(
                    after, jnp.where(sub < ROWS - k, pltpu.roll(after, ROWS - k, axis=0), ROWS)
                )
            has_f = before >= 0
            has_b = after < ROWS
            at_f = jnp.maximum(before, 0)
            at_b = jnp.minimum(after, ROWS - 1)

            def sides(x, b, sign):
                p, r = row_of(b, j)
                f = jnp.take_along_axis(x, at_f, axis=0)
                n = jnp.take_along_axis(x, at_b, axis=0)
                f = jnp.where(has_f, f, spread(enter[g, 0, p, r, :]))
                n = jnp.where(has_b, n, spread(sign * enter[g, 1, p, r, :]))
                return f, n

            prev, following = sides(day_col, bands, -1.0)
            span = following - prev
            weight = (day_col - prev) / jnp.where(span == 0.0, 1.0, span)
            for b in range(bands):
                f, n = sides(xv[b, :, cols], b, 1.0)
                out_ref[b, :, cols] = f + weight * (n - f)

    loaded = 0
    for m, (start, count) in enumerate(messages):
        while loaded < len(loads) and loads[loaded][0] < start + count:
            load_v(loaded).wait()
            load_x(loaded).wait()
            loaded += 1
        over(m, summarize)
        if m == 0:
            pl.semaphore_wait(barrier, len(pair) + len(rows))
        swap(0, m).start()

    for stage, m in arrival_order(messages):
        if stage < 2:
            swap(stage, m).wait_recv()
            over(m, functools.partial(merge_pair, stage))
            if stage == 0:
                swap(1, m).start()
            else:
                for d in range(SIDE - 1):
                    to_row(d, m).start()
            over(m, functools.partial(note_pair, stage))
        else:
            from_rows(pl.ds(*messages[m]), m).wait_recv()
            over(m, complete)

    for stage in range(2):
        pltpu.make_async_remote_copy(
            src_ref=own.at[stage],
            dst_ref=come.at[stage],
            send_sem=send_sem.at[stage],
            recv_sem=recv_sem.at[stage, 0],
            device_id=pair[stage],
            device_id_type=MESH,
        ).wait_send()
    from_rows(pl.ds(0, groups), 0).wait_send()


def body(reflectance, validity, day_number):
    dates, bands, pixels = reflectance.shape
    groups = pixels // (TILES * LANES)
    packs = (bands + 1) // 2
    messages, loads = len(spans(SHARES, groups)), len(spans(LOADS, groups))
    hbm = pl.BlockSpec(memory_space=pltpu.HBM)
    filled = pl.pallas_call(
        functools.partial(scan_fill, bands, groups),
        out_shape=pltpu.VMEM((bands, dates, pixels), jnp.float32),
        in_specs=[hbm, hbm, hbm],
        out_specs=pl.BlockSpec(memory_space=pltpu.VMEM),
        scratch_shapes=[
            pltpu.SMEM((dates,), jnp.int32),
            pltpu.VMEM((bands, dates, pixels), jnp.float32),
            pltpu.VMEM((dates, pixels), jnp.int32),
            pltpu.VMEM((3, groups, 2, packs, ROWS, LANES), jnp.float32),
            pltpu.VMEM((2, groups, 2, packs, ROWS, LANES), jnp.float32),
            pltpu.VMEM((groups, SIDE - 1, packs, ROWS, LANES), jnp.float32),
            pltpu.VMEM((groups, 2, packs, ROWS, LANES), jnp.float32),
            pltpu.SemaphoreType.DMA,
            pltpu.SemaphoreType.DMA((loads,)),
            pltpu.SemaphoreType.DMA((loads,)),
            pltpu.SemaphoreType.DMA((3,)),
            pltpu.SemaphoreType.DMA((3, messages)),
        ],
        compiler_params=pltpu.CompilerParams(
            collective_id=0, has_side_effects=True, vmem_limit_bytes=(62 << 20) - 65536
        ),
        name="scan_fill",
    )(day_number, jnp.transpose(reflectance, (1, 0, 2)), validity)
    return jnp.transpose(filled, (1, 0, 2))


def solution(mesh):
    torus = Mesh(
        mesh.devices.reshape(4, 4, mesh.shape["pix"], mesh.shape["tile"]),
        ("date_0", "date_1", "pix", "tile"),
    )
    placed = (P(DATE, None, ("tile", "pix")), P(DATE, ("tile", "pix")), P(DATE))
    return jax.shard_map(
        body, mesh=torus, in_specs=placed, out_specs=P(DATE, None, ("tile", "pix")), check_vma=False
    )
```

```python
import functools

import jax
import jax.numpy as jnp
from jax import lax
from jax.experimental import pallas as pl
from jax.experimental.pallas import tpu as pltpu
from jax.sharding import Mesh
from jax.sharding import PartitionSpec as P

MESH = pl.DeviceIdType.MESH
DATE = ("date_0", "date_1")
LANES = 128
ROWS = 8
TILES = 4
SIDE = 4
NONE = -1073741824.0
STRAIGHT, TURNED = 1, 2
SHARES = (-1, 1, 2, 2, 2, 2, 1, 1, -1)
LOADS = (2, 6, 8)
UNIT, HOP, FAR = 0.35, 3.0, 4.0
EARLY, MIDDLE = 5, 10
TURN = 16


def pieces(shares, groups):
    if sum(abs(s) for s in shares) != groups:
        return [(g, 1) for g in range(groups)]
    starts, at = [], 0
    for share in shares:
        starts.append((at, abs(share)))
        at += abs(share)
    return starts


def plan(groups):
    across, turned = (STRAIGHT, TURNED) if groups > STRAIGHT + TURNED else (1, 1)
    hyper = groups - across - turned
    parts = pieces(SHARES, hyper)
    split = [s < 0 for s in SHARES] if len(parts) == len(SHARES) else [False] * len(parts)
    messages, owner = [], []
    for r, (start, count) in enumerate(parts):
        for side in (0, 1) if split[r] else (None,):
            messages.append((start, count, side or 0, 2 if side is None else 1))
            owner.append(r)
    rows = [*parts, (hyper, across), (hyper + across, turned)]
    load = 2 * across * UNIT
    events, first, second = [], 0.0, 2 * load
    ready, straight = [], 0.0
    for i, m in enumerate(messages):
        if i == min(EARLY, len(messages) - 1):
            first += load
        if i == min(MIDDLE, len(messages) - 1):
            first += load
            straight = first + HOP
        first += m[1] * m[3] * UNIT
        ready.append(first + HOP)
        events.append((ready[i], 0, i))
    events.append((straight, 2, 0))
    done = [0.0] * (len(rows) - 1)
    done[-1] = straight
    for i, m in enumerate(messages):
        second = max(second, ready[i]) + m[1] * m[3] * UNIT
        events.append((second + HOP, 1, i))
        done[owner[i]] = second + HOP
    link = 0.0
    for r in sorted(range(len(done)), key=lambda r: done[r]):
        link = max(link, done[r]) + 2 * UNIT * rows[r][1]
        events.append((link + FAR, 3, r))
    events.append((TURN, 4, 0))
    events.append((max(TURN, first, second) + 4 * turned * UNIT + FAR, 5, 0))
    return messages, owner, rows, [(kind, i) for _, kind, i in sorted(events)]


def scan_fill(
    bands,
    groups,
    days_hbm,
    x_hbm,
    v_hbm,
    out_ref,
    days,
    xv,
    vv,
    own,
    come,
    come_x,
    come_y,
    enter,
    day_sem,
    x_sem,
    v_sem,
    send_sem,
    recv_sem,
):
    width = TILES * LANES
    packs = (bands + 1) // 2
    loads = pieces(LOADS, groups)
    messages, owner, row_parts, order = plan(groups)
    straight, turned = row_parts[-2:]
    places = (pl.ds(0, straight[1]), pl.ds(straight[1], turned[1]))
    yi = lax.axis_index(DATE[0])
    xi = lax.axis_index(DATE[1])
    pair = ({DATE[1]: xi + 1 - 2 * lax.rem(xi, 2)}, {DATE[1]: 3 - xi})
    taken = (1 - lax.rem(xi, 2), 1 - xi // 2)
    rows = [{DATE[0]: lax.rem(yi + d, SIDE)} for d in range(1, SIDE)]
    row_gives = [(yi + d) // SIDE for d in range(1, SIDE)]
    row_takes = [1 - (yi + SIDE - d) // SIDE for d in range(1, SIDE)]
    crossing = (pair[1], {DATE[1]: lax.rem(xi + 2, SIDE)}, pair[0])
    cross_takes = (1 - xi // 2, 1 - xi // 2, 1 - lax.rem(xi, 2))

    def load_x(i):
        cols = pl.ds(loads[i][0] * width, loads[i][1] * width)
        return pltpu.make_async_copy(x_hbm.at[:, :, cols], xv.at[:, :, cols], x_sem.at[i])

    def load_v(i):
        cols = pl.ds(loads[i][0] * width, loads[i][1] * width)
        return pltpu.make_async_copy(v_hbm.at[:, cols], vv.at[:, cols], v_sem.at[i])

    def swap(stage, m):
        start, count, side, sides = messages[m]
        part, which = pl.ds(start, count), pl.ds(side, sides)
        return pltpu.make_async_remote_copy(
            src_ref=own.at[stage, part, which],
            dst_ref=come.at[stage, part, which],
            send_sem=send_sem.at[stage],
            recv_sem=recv_sem.at[stage * len(messages) + m],
            device_id=pair[stage],
            device_id_type=MESH,
        )

    def cross(turn, i):
        return pltpu.make_async_remote_copy(
            src_ref=own.at[1 + cross_takes[i], pl.ds(*turned)] if turn else own.at[0, pl.ds(*straight)],
            dst_ref=come_x.at[i, places[turn]],
            send_sem=send_sem.at[2],
            recv_sem=recv_sem.at[2 * len(messages) + turn],
            device_id=crossing[i],
            device_id_type=MESH,
        )

    def crossed(part, turn):
        return pltpu.make_async_remote_copy(
            src_ref=part,
            dst_ref=part,
            send_sem=send_sem.at[2],
            recv_sem=recv_sem.at[2 * len(messages) + turn],
            device_id=crossing[0],
            device_id_type=MESH,
        )

    def row_sem(r):
        return recv_sem.at[2 * len(messages) + 2 + r]

    def to_row(d, r):
        part = pl.ds(*row_parts[r])
        return pltpu.make_async_remote_copy(
            src_ref=own.at[0 if r == len(row_parts) - 1 else 2, part, row_gives[d]],
            dst_ref=come_y.at[part, d],
            send_sem=send_sem.at[3],
            recv_sem=row_sem(r),
            device_id=rows[d],
            device_id_type=MESH,
        )

    def from_rows(part, r):
        return pltpu.make_async_remote_copy(
            src_ref=come_y.at[part],
            dst_ref=come_y.at[part],
            send_sem=send_sem.at[3],
            recv_sem=row_sem(r),
            device_id=rows[0],
            device_id_type=MESH,
        )

    barrier = pltpu.get_barrier_semaphore()
    for who in (*crossing, *rows):
        pl.semaphore_signal(barrier, inc=1, device_id=who, device_id_type=MESH)
    day_copy = pltpu.make_async_copy(days_hbm, days, day_sem)
    day_copy.start()
    for i in range(len(loads)):
        load_v(i).start()
        load_x(i).start()

    day_copy.wait()
    sub = lax.broadcasted_iota(jnp.int32, (ROWS, LANES), 0)
    day_col = jnp.zeros((ROWS, LANES), jnp.float32)
    for t in range(ROWS):
        day_col = jnp.where(sub == t, days[t].astype(jnp.float32), day_col)
    key_rows = sub >= TILES

    def lanes_of(g, j):
        return pl.ds(pl.multiple_of(g * width + j * LANES, LANES), LANES)

    def key_of(pack):
        return jnp.where(key_rows, pack, pltpu.roll(pack, TILES, axis=0))

    def spread(row):
        return jnp.broadcast_to(row, (ROWS, LANES))

    def row_of(band, j):
        return band // 2, pl.ds((band % 2) * TILES + j, 1)

    def over(start, count, work):
        if count == 1:
            work(start)
        else:
            pl.loop(start, start + count)(work)

    def summarize(g):
        for j in range(TILES):
            cols = lanes_of(g, j)
            live = vv[:, cols] > 0
            last = jnp.max(jnp.where(live, day_col, NONE), axis=0, keepdims=True)
            first = jnp.max(jnp.where(live, -day_col, NONE), axis=0, keepdims=True)
            at_last = day_col == spread(last)
            at_first = -day_col == spread(first)
            for b in range(bands):
                x = xv[b, :, cols]
                p, r = row_of(b, j)
                own[0, g, 0, p, r, :] = jnp.sum(jnp.where(at_last, x, 0.0), axis=0, keepdims=True)
                own[0, g, 1, p, r, :] = jnp.sum(jnp.where(at_first, x, 0.0), axis=0, keepdims=True)
            p, r = row_of(bands, j)
            own[0, g, 0, p, r, :] = last
            own[0, g, 1, p, r, :] = first

    def merge_pair(stage, sides, g):
        for side in sides:
            take = key_of(come[stage, g, side, packs - 1]) > key_of(own[stage, g, side, packs - 1])
            for p in range(packs):
                own[stage + 1, g, side, p] = jnp.where(
                    take, come[stage, g, side, p], own[stage, g, side, p]
                )

    def enter_less(g, side, packs_of):
        take = key_of(packs_of(packs - 1)) > key_of(enter[g, side, packs - 1])
        for p in range(packs):
            enter[g, side, p] = jnp.where(take, packs_of(p), enter[g, side, p])

    def clear(g, side):
        for p in range(packs):
            enter[g, side, p] = jnp.where(key_rows, NONE if p == packs - 1 else 0.0, 0.0)

    def note_pair(g):
        side = taken[0]
        clear(g, 1 - side)
        for p in range(packs):
            enter[g, side, p] = come[0, g, side, p]
        enter_less(g, taken[1], lambda p: come[1, g, taken[1], p])

    def merge_cross(k):
        g = straight[0] + k
        for side in range(2):
            best = [own[0, g, side, p] for p in range(packs)]
            for i in range(SIDE - 1):
                take = key_of(come_x[i, k, side, packs - 1]) > key_of(best[-1])
                best = [jnp.where(take, come_x[i, k, side, p], best[p]) for p in range(packs)]
            for p in range(packs):
                own[2, g, side, p] = best[p]

    def note_cross(k):
        g = straight[0] + k
        for side in range(2):
            clear(g, side)
        for i in range(SIDE - 1):
            enter_less(g, cross_takes[i], lambda p: come_x[i, k, cross_takes[i], p])

    def note_rows(g):
        for d in range(SIDE - 1):
            enter_less(g, row_takes[d], lambda p: come_y[g, d, p])

    def turn_along(k):
        g = turned[0] + k
        for side in range(2):
            clear(g, side)
        note_rows(g)
        for side in range(2):
            take = key_of(own[0, g, side, packs - 1]) > key_of(enter[g, side, packs - 1])
            for p in range(packs):
                before = enter[g, side, p]
                own[2 - side, g, side, p] = jnp.where(take, own[0, g, side, p], before)
                own[1 + side, g, side, p] = before

    def complete_rows(g):
        note_rows(g)
        complete(g)

    def complete_turned(k):
        g = turned[0] + k
        for i in range(SIDE - 1):
            for side in range(2):
                enter_less(g, side, lambda p: come_x[i, straight[1] + k, side, p])
        complete(g)

    def complete(g):
        has = [key_of(enter[g, s, packs - 1]) > NONE for s in range(2)]
        mine = [key_of(own[0, g, s, packs - 1]) > NONE for s in range(2)]
        for p in range(packs):
            ends = [enter[g, s, p] for s in range(2)]
            other = [jnp.where(mine[s], own[0, g, s, p], ends[s]) for s in range(2)]
            if p == packs - 1:
                other = [jnp.where(key_rows, -o, o) for o in other]
            for s in range(2):
                enter[g, s, p] = jnp.where(has[s], ends[s], other[1 - s])
        for j in range(TILES):
            cols = lanes_of(g, j)
            live = vv[:, cols] > 0
            before = jnp.where(live, sub, -1)
            after = jnp.where(live, sub, ROWS)
            for k in (1, 2, 4):
                before = jnp.maximum(
                    before, jnp.where(sub >= k, pltpu.roll(before, k, axis=0), -1)
                )
                after = jnp.minimum(
                    after, jnp.where(sub < ROWS - k, pltpu.roll(after, ROWS - k, axis=0), ROWS)
                )
            has_f = before >= 0
            has_b = after < ROWS
            at_f = jnp.maximum(before, 0)
            at_b = jnp.minimum(after, ROWS - 1)

            def sides(x, b, sign):
                p, r = row_of(b, j)
                f = jnp.take_along_axis(x, at_f, axis=0)
                n = jnp.take_along_axis(x, at_b, axis=0)
                f = jnp.where(has_f, f, spread(enter[g, 0, p, r, :]))
                n = jnp.where(has_b, n, spread(sign * enter[g, 1, p, r, :]))
                return f, n

            prev, following = sides(day_col, bands, -1.0)
            span = following - prev
            weight = (day_col - prev) / jnp.where(span == 0.0, 1.0, span)
            for b in range(bands):
                f, n = sides(xv[b, :, cols], b, 1.0)
                out_ref[b, :, cols] = f + weight * (n - f)

    loaded = 0

    def summarize_part(start, count):
        nonlocal loaded
        while loaded < len(loads) and loads[loaded][0] < start + count:
            load_v(loaded).wait()
            load_x(loaded).wait()
            loaded += 1
        over(start, count, summarize)

    summarized = set()
    for m, (start, count, _, _) in enumerate(messages):
        if m == min(MIDDLE, len(messages) - 1):
            cross(0, 2).start()
        if start not in summarized:
            summarize_part(start, count)
            summarized.add(start)
        if m == 0:
            pl.semaphore_wait(barrier, len(pair) + len(rows) + 1)
        swap(0, m).start()
        if m == min(EARLY, len(messages) - 1) - 1 or len(messages) == 1:
            summarize_part(*turned)
            for d in range(SIDE - 1):
                to_row(d, len(row_parts) - 1).start()
            summarize_part(*straight)
            cross(0, 0).start()
            cross(0, 1).start()

    for kind, i in order:
        if kind < 2:
            start, count, side, sides = messages[i]
            swap(kind, i).wait_recv()
            over(start, count, functools.partial(merge_pair, kind, range(side, side + sides)))
            if kind == 0:
                swap(1, i).start()
            else:
                for d in range(SIDE - 1):
                    if sides == 2:
                        to_row(d, owner[i]).start()
                    else:
                        pl.when(row_gives[d] == side)(to_row(d, owner[i]).start)
                if side + sides == 2:
                    over(start, count, note_pair)
        elif kind == 2:
            crossed(come_x.at[:, places[0]], 0).wait_recv()
            over(0, straight[1], merge_cross)
            for d in range(SIDE - 1):
                to_row(d, len(row_parts) - 2).start()
            over(0, straight[1], note_cross)
        elif kind == 3:
            from_rows(pl.ds(*row_parts[i]), i).wait_recv()
            over(*row_parts[i], complete_rows)
        elif kind == 4:
            from_rows(pl.ds(*turned), len(row_parts) - 1).wait_recv()
            over(0, turned[1], turn_along)
            for k in range(SIDE - 1):
                cross(1, k).start()
        else:
            crossed(come_x.at[:, places[1]], 1).wait_recv()
            over(0, turned[1], complete_turned)

    for stage in range(2):
        part = pl.ds(0, straight[0])
        pltpu.make_async_remote_copy(
            src_ref=own.at[stage, part],
            dst_ref=come.at[stage, part],
            send_sem=send_sem.at[stage],
            recv_sem=recv_sem.at[0],
            device_id=pair[stage],
            device_id_type=MESH,
        ).wait_send()
    crossed(come_x, 0).wait_send()
    from_rows(pl.ds(0, groups), 0).wait_send()


def body(reflectance, validity, day_number):
    dates, bands, pixels = reflectance.shape
    groups = pixels // (TILES * LANES)
    packs = (bands + 1) // 2
    messages, _, rows, _ = plan(groups)
    loads = len(pieces(LOADS, groups))
    hbm = pl.BlockSpec(memory_space=pltpu.HBM)
    filled = pl.pallas_call(
        functools.partial(scan_fill, bands, groups),
        out_shape=pltpu.VMEM((bands, dates, pixels), jnp.float32),
        in_specs=[hbm, hbm, hbm],
        out_specs=pl.BlockSpec(memory_space=pltpu.VMEM),
        scratch_shapes=[
            pltpu.SMEM((dates,), jnp.int32),
            pltpu.VMEM((bands, dates, pixels), jnp.float32),
            pltpu.VMEM((dates, pixels), jnp.int32),
            pltpu.VMEM((3, groups, 2, packs, ROWS, LANES), jnp.float32),
            pltpu.VMEM((2, groups, 2, packs, ROWS, LANES), jnp.float32),
            pltpu.VMEM((SIDE - 1, rows[-2][1] + rows[-1][1], 2, packs, ROWS, LANES), jnp.float32),
            pltpu.VMEM((groups, SIDE - 1, packs, ROWS, LANES), jnp.float32),
            pltpu.VMEM((groups, 2, packs, ROWS, LANES), jnp.float32),
            pltpu.SemaphoreType.DMA,
            pltpu.SemaphoreType.DMA((loads,)),
            pltpu.SemaphoreType.DMA((loads,)),
            pltpu.SemaphoreType.DMA((4,)),
            pltpu.SemaphoreType.DMA((2 * len(messages) + 2 + len(rows),)),
        ],
        compiler_params=pltpu.CompilerParams(
            collective_id=0, has_side_effects=True, vmem_limit_bytes=(62 << 20) - 65536
        ),
        name="scan_fill",
    )(day_number, jnp.transpose(reflectance, (1, 0, 2)), validity)
    return jnp.transpose(filled, (1, 0, 2))


def solution(mesh):
    torus = Mesh(
        mesh.devices.reshape(4, 4, mesh.shape["pix"], mesh.shape["tile"]),
        ("date_0", "date_1", "pix", "tile"),
    )
    placed = (P(DATE, None, ("tile", "pix")), P(DATE, ("tile", "pix")), P(DATE))
    return jax.shard_map(
        body, mesh=torus, in_specs=placed, out_specs=P(DATE, None, ("tile", "pix")), check_vma=False
    )
```

```python
import functools

import jax
import jax.numpy as jnp
from jax import lax
from jax.experimental import pallas as pl
from jax.experimental.pallas import tpu as pltpu
from jax.sharding import Mesh
from jax.sharding import PartitionSpec as P

MESH = pl.DeviceIdType.MESH
DATE = ("date_0", "date_1")
LANES = 128
ROWS = 8
TILES = 4
FAR_FIRST = (1, 0, 2)
SIDE = 4
NONE = -1073741824.0
STRAIGHT, TURNED = 1, 2
SHARES = (-1, 1, 2, 2, 2, 2, 1, -1, -1)
LOADS = (2, 6, 8)
UNIT, HOP, FAR = 0.35, 3.0, 4.0
EARLY, MIDDLE = 5, 11
TURN = 16


def pieces(shares, groups):
    if sum(abs(s) for s in shares) != groups:
        return [(g, 1) for g in range(groups)]
    starts, at = [], 0
    for share in shares:
        starts.append((at, abs(share)))
        at += abs(share)
    return starts


def plan(groups):
    across, turned = (STRAIGHT, TURNED) if groups > STRAIGHT + TURNED else (1, 1)
    hyper = groups - across - turned
    parts = pieces(SHARES, hyper)
    split = [s < 0 for s in SHARES] if len(parts) == len(SHARES) else [False] * len(parts)
    messages, owner = [], []
    for r, (start, count) in enumerate(parts):
        for side in (0, 1) if split[r] else (None,):
            messages.append((start, count, side or 0, 2 if side is None else 1))
            owner.append(r)
    rows = [*parts, (hyper, across), (hyper + across, turned)]
    load = 2 * across * UNIT
    events, first, second = [], 0.0, 2 * load
    ready, straight = [], 0.0
    for i, m in enumerate(messages):
        if i == min(EARLY, len(messages) - 1):
            first += load
        if i == min(MIDDLE, len(messages) - 1):
            first += load
            straight = first + HOP
        first += m[1] * m[3] * UNIT
        ready.append(first + HOP)
        events.append((ready[i], 0, i))
    events.append((straight, 2, 0))
    done = [0.0] * (len(rows) - 1)
    done[-1] = straight
    for i, m in enumerate(messages):
        second = max(second, ready[i]) + m[1] * m[3] * UNIT
        events.append((second + HOP, 1, i))
        done[owner[i]] = second + HOP
    link = 0.0
    for r in sorted(range(len(done)), key=lambda r: done[r]):
        link = max(link, done[r]) + 2 * UNIT * rows[r][1]
        events.append((link + FAR, 3, r))
    events.append((TURN, 4, 0))
    events.append((max(TURN, first, second) + 4 * turned * UNIT + FAR, 5, 0))
    return messages, owner, rows, [(kind, i) for _, kind, i in sorted(events)]


def scan_fill(
    bands,
    groups,
    days_hbm,
    x_hbm,
    v_hbm,
    out_ref,
    days,
    xv,
    vv,
    own,
    come,
    come_x,
    come_y,
    enter,
    day_sem,
    x_sem,
    v_sem,
    send_sem,
    recv_sem,
):
    width = TILES * LANES
    packs = (bands + 1) // 2
    loads = pieces(LOADS, groups)
    messages, owner, row_parts, order = plan(groups)
    straight, turned = row_parts[-2:]
    places = (pl.ds(0, straight[1]), pl.ds(straight[1], turned[1]))
    yi = lax.axis_index(DATE[0])
    xi = lax.axis_index(DATE[1])
    pair = ({DATE[1]: xi + 1 - 2 * lax.rem(xi, 2)}, {DATE[1]: 3 - xi})
    taken = (1 - lax.rem(xi, 2), 1 - xi // 2)
    rows = [{DATE[0]: lax.rem(yi + d, SIDE)} for d in range(1, SIDE)]
    row_gives = [(yi + d) // SIDE for d in range(1, SIDE)]
    row_takes = [1 - (yi + SIDE - d) // SIDE for d in range(1, SIDE)]
    crossing = (pair[1], {DATE[1]: lax.rem(xi + 2, SIDE)}, pair[0])
    cross_takes = (1 - xi // 2, 1 - xi // 2, 1 - lax.rem(xi, 2))

    def load_x(i):
        cols = pl.ds(loads[i][0] * width, loads[i][1] * width)
        return pltpu.make_async_copy(x_hbm.at[:, :, cols], xv.at[:, :, cols], x_sem.at[i])

    def load_v(i):
        cols = pl.ds(loads[i][0] * width, loads[i][1] * width)
        return pltpu.make_async_copy(v_hbm.at[:, cols], vv.at[:, cols], v_sem.at[i])

    def swap(stage, m):
        start, count, side, sides = messages[m]
        part, which = pl.ds(start, count), pl.ds(side, sides)
        return pltpu.make_async_remote_copy(
            src_ref=own.at[stage, part, which],
            dst_ref=come.at[stage, part, which],
            send_sem=send_sem.at[stage],
            recv_sem=recv_sem.at[stage * len(messages) + m],
            device_id=pair[stage],
            device_id_type=MESH,
        )

    def cross(turn, i):
        return pltpu.make_async_remote_copy(
            src_ref=own.at[1 + cross_takes[i], pl.ds(*turned)] if turn else own.at[0, pl.ds(*straight)],
            dst_ref=come_x.at[i, places[turn]],
            send_sem=send_sem.at[2],
            recv_sem=recv_sem.at[2 * len(messages) + turn],
            device_id=crossing[i],
            device_id_type=MESH,
        )

    def crossed(part, turn):
        return pltpu.make_async_remote_copy(
            src_ref=part,
            dst_ref=part,
            send_sem=send_sem.at[2],
            recv_sem=recv_sem.at[2 * len(messages) + turn],
            device_id=crossing[0],
            device_id_type=MESH,
        )

    def row_sem(r):
        return recv_sem.at[2 * len(messages) + 2 + r]

    def to_row(d, r):
        part = pl.ds(*row_parts[r])
        return pltpu.make_async_remote_copy(
            src_ref=own.at[0 if r == len(row_parts) - 1 else 2, part, row_gives[d]],
            dst_ref=come_y.at[part, d],
            send_sem=send_sem.at[3],
            recv_sem=row_sem(r),
            device_id=rows[d],
            device_id_type=MESH,
        )

    def from_rows(part, r):
        return pltpu.make_async_remote_copy(
            src_ref=come_y.at[part],
            dst_ref=come_y.at[part],
            send_sem=send_sem.at[3],
            recv_sem=row_sem(r),
            device_id=rows[0],
            device_id_type=MESH,
        )

    barrier = pltpu.get_barrier_semaphore()
    for who in (*crossing, *rows):
        pl.semaphore_signal(barrier, inc=1, device_id=who, device_id_type=MESH)
    day_copy = pltpu.make_async_copy(days_hbm, days, day_sem)
    day_copy.start()
    for i in range(len(loads)):
        load_v(i).start()
        load_x(i).start()

    day_copy.wait()
    sub = lax.broadcasted_iota(jnp.int32, (ROWS, LANES), 0)
    day_col = jnp.zeros((ROWS, LANES), jnp.float32)
    for t in range(ROWS):
        day_col = jnp.where(sub == t, days[t].astype(jnp.float32), day_col)
    key_rows = sub >= TILES

    def lanes_of(g, j):
        return pl.ds(pl.multiple_of(g * width + j * LANES, LANES), LANES)

    def key_of(pack):
        return jnp.where(key_rows, pack, pltpu.roll(pack, TILES, axis=0))

    def spread(row):
        return jnp.broadcast_to(row, (ROWS, LANES))

    def row_of(band, j):
        return band // 2, pl.ds((band % 2) * TILES + j, 1)

    def over(start, count, work):
        if count == 1:
            work(start)
        else:
            pl.loop(start, start + count)(work)

    def summarize(g):
        for j in range(TILES):
            cols = lanes_of(g, j)
            live = vv[:, cols] > 0
            last = jnp.max(jnp.where(live, day_col, NONE), axis=0, keepdims=True)
            first = jnp.max(jnp.where(live, -day_col, NONE), axis=0, keepdims=True)
            at_last = day_col == spread(last)
            at_first = -day_col == spread(first)
            for b in range(bands):
                x = xv[b, :, cols]
                p, r = row_of(b, j)
                own[0, g, 0, p, r, :] = jnp.sum(jnp.where(at_last, x, 0.0), axis=0, keepdims=True)
                own[0, g, 1, p, r, :] = jnp.sum(jnp.where(at_first, x, 0.0), axis=0, keepdims=True)
            p, r = row_of(bands, j)
            own[0, g, 0, p, r, :] = last
            own[0, g, 1, p, r, :] = first

    def merge_pair(stage, sides, g):
        for side in sides:
            take = key_of(come[stage, g, side, packs - 1]) > key_of(own[stage, g, side, packs - 1])
            for p in range(packs):
                own[stage + 1, g, side, p] = jnp.where(
                    take, come[stage, g, side, p], own[stage, g, side, p]
                )

    def enter_less(g, side, packs_of):
        take = key_of(packs_of(packs - 1)) > key_of(enter[g, side, packs - 1])
        for p in range(packs):
            enter[g, side, p] = jnp.where(take, packs_of(p), enter[g, side, p])

    def clear(g, side):
        for p in range(packs):
            enter[g, side, p] = jnp.where(key_rows, NONE if p == packs - 1 else 0.0, 0.0)

    def note_pair(g):
        side = taken[0]
        clear(g, 1 - side)
        for p in range(packs):
            enter[g, side, p] = come[0, g, side, p]
        enter_less(g, taken[1], lambda p: come[1, g, taken[1], p])

    def merge_cross(k):
        g = straight[0] + k
        for side in range(2):
            best = [own[0, g, side, p] for p in range(packs)]
            for i in range(SIDE - 1):
                take = key_of(come_x[i, k, side, packs - 1]) > key_of(best[-1])
                best = [jnp.where(take, come_x[i, k, side, p], best[p]) for p in range(packs)]
            for p in range(packs):
                own[2, g, side, p] = best[p]

    def note_cross(k):
        g = straight[0] + k
        for side in range(2):
            clear(g, side)
        for i in range(SIDE - 1):
            enter_less(g, cross_takes[i], lambda p: come_x[i, k, cross_takes[i], p])

    def note_rows(g):
        for d in range(SIDE - 1):
            enter_less(g, row_takes[d], lambda p: come_y[g, d, p])

    def turn_along(k):
        g = turned[0] + k
        for side in range(2):
            clear(g, side)
        note_rows(g)
        for side in range(2):
            take = key_of(own[0, g, side, packs - 1]) > key_of(enter[g, side, packs - 1])
            for p in range(packs):
                before = enter[g, side, p]
                own[2 - side, g, side, p] = jnp.where(take, own[0, g, side, p], before)
                own[1 + side, g, side, p] = before

    def complete_rows(g):
        note_rows(g)
        complete(g)

    def complete_turned(k):
        g = turned[0] + k
        for i in range(SIDE - 1):
            for side in range(2):
                enter_less(g, side, lambda p: come_x[i, straight[1] + k, side, p])
        complete(g)

    def complete(g):
        has = [key_of(enter[g, s, packs - 1]) > NONE for s in range(2)]
        mine = [key_of(own[0, g, s, packs - 1]) > NONE for s in range(2)]
        for p in range(packs):
            ends = [enter[g, s, p] for s in range(2)]
            other = [jnp.where(mine[s], own[0, g, s, p], ends[s]) for s in range(2)]
            if p == packs - 1:
                other = [jnp.where(key_rows, -o, o) for o in other]
            for s in range(2):
                enter[g, s, p] = jnp.where(has[s], ends[s], other[1 - s])
        for j in range(TILES):
            cols = lanes_of(g, j)
            live = vv[:, cols] > 0
            before = jnp.where(live, sub, -1)
            after = jnp.where(live, sub, ROWS)
            for k in (1, 2, 4):
                before = jnp.maximum(
                    before, jnp.where(sub >= k, pltpu.roll(before, k, axis=0), -1)
                )
                after = jnp.minimum(
                    after, jnp.where(sub < ROWS - k, pltpu.roll(after, ROWS - k, axis=0), ROWS)
                )
            has_f = before >= 0
            has_b = after < ROWS
            at_f = jnp.maximum(before, 0)
            at_b = jnp.minimum(after, ROWS - 1)

            def sides(x, b, sign):
                p, r = row_of(b, j)
                f = jnp.take_along_axis(x, at_f, axis=0)
                n = jnp.take_along_axis(x, at_b, axis=0)
                f = jnp.where(has_f, f, spread(enter[g, 0, p, r, :]))
                n = jnp.where(has_b, n, spread(sign * enter[g, 1, p, r, :]))
                return f, n

            prev, following = sides(day_col, bands, -1.0)
            span = following - prev
            weight = (day_col - prev) / jnp.where(span == 0.0, 1.0, span)
            for b in range(bands):
                f, n = sides(xv[b, :, cols], b, 1.0)
                out_ref[b, :, cols] = f + weight * (n - f)

    loaded = 0

    def summarize_part(start, count):
        nonlocal loaded
        while loaded < len(loads) and loads[loaded][0] < start + count:
            load_v(loaded).wait()
            load_x(loaded).wait()
            loaded += 1
        over(start, count, summarize)

    summarized = set()
    for m, (start, count, _, _) in enumerate(messages):
        if m == min(MIDDLE, len(messages) - 1):
            cross(0, 2).start()
        if start not in summarized:
            summarize_part(start, count)
            summarized.add(start)
        if m == 0:
            pl.semaphore_wait(barrier, len(pair) + len(rows) + 1)
        swap(0, m).start()
        if m == min(EARLY, len(messages) - 1) - 1 or len(messages) == 1:
            summarize_part(*turned)
            for d in range(SIDE - 1):
                to_row(d, len(row_parts) - 1).start()
            summarize_part(*straight)
            cross(0, 0).start()
            cross(0, 1).start()

    for kind, i in order:
        if kind < 2:
            start, count, side, sides = messages[i]
            swap(kind, i).wait_recv()
            over(start, count, functools.partial(merge_pair, kind, range(side, side + sides)))
            if kind == 0:
                swap(1, i).start()
            else:
                for d in FAR_FIRST:
                    if sides == 2:
                        to_row(d, owner[i]).start()
                    else:
                        pl.when(row_gives[d] == side)(to_row(d, owner[i]).start)
                if side + sides == 2:
                    over(start, count, note_pair)
        elif kind == 2:
            crossed(come_x.at[:, places[0]], 0).wait_recv()
            over(0, straight[1], merge_cross)
            for d in FAR_FIRST:
                to_row(d, len(row_parts) - 2).start()
            over(0, straight[1], note_cross)
        elif kind == 3:
            from_rows(pl.ds(*row_parts[i]), i).wait_recv()
            over(*row_parts[i], complete_rows)
        elif kind == 4:
            from_rows(pl.ds(*turned), len(row_parts) - 1).wait_recv()
            over(0, turned[1], turn_along)
            for k in range(SIDE - 1):
                cross(1, k).start()
        else:
            crossed(come_x.at[:, places[1]], 1).wait_recv()
            over(0, turned[1], complete_turned)

    for stage in range(2):
        part = pl.ds(0, straight[0])
        pltpu.make_async_remote_copy(
            src_ref=own.at[stage, part],
            dst_ref=come.at[stage, part],
            send_sem=send_sem.at[stage],
            recv_sem=recv_sem.at[0],
            device_id=pair[stage],
            device_id_type=MESH,
        ).wait_send()
    crossed(come_x, 0).wait_send()
    from_rows(pl.ds(0, groups), 0).wait_send()


def body(reflectance, validity, day_number):
    dates, bands, pixels = reflectance.shape
    groups = pixels // (TILES * LANES)
    packs = (bands + 1) // 2
    messages, _, rows, _ = plan(groups)
    loads = len(pieces(LOADS, groups))
    hbm = pl.BlockSpec(memory_space=pltpu.HBM)
    filled = pl.pallas_call(
        functools.partial(scan_fill, bands, groups),
        out_shape=pltpu.VMEM((bands, dates, pixels), jnp.float32),
        in_specs=[hbm, hbm, hbm],
        out_specs=pl.BlockSpec(memory_space=pltpu.VMEM),
        scratch_shapes=[
            pltpu.SMEM((dates,), jnp.int32),
            pltpu.VMEM((bands, dates, pixels), jnp.float32),
            pltpu.VMEM((dates, pixels), jnp.int32),
            pltpu.VMEM((3, groups, 2, packs, ROWS, LANES), jnp.float32),
            pltpu.VMEM((2, groups, 2, packs, ROWS, LANES), jnp.float32),
            pltpu.VMEM((SIDE - 1, rows[-2][1] + rows[-1][1], 2, packs, ROWS, LANES), jnp.float32),
            pltpu.VMEM((groups, SIDE - 1, packs, ROWS, LANES), jnp.float32),
            pltpu.VMEM((groups, 2, packs, ROWS, LANES), jnp.float32),
            pltpu.SemaphoreType.DMA,
            pltpu.SemaphoreType.DMA((loads,)),
            pltpu.SemaphoreType.DMA((loads,)),
            pltpu.SemaphoreType.DMA((4,)),
            pltpu.SemaphoreType.DMA((2 * len(messages) + 2 + len(rows),)),
        ],
        compiler_params=pltpu.CompilerParams(
            collective_id=0, has_side_effects=True, vmem_limit_bytes=(62 << 20) - 65536
        ),
        name="scan_fill",
    )(day_number, jnp.transpose(reflectance, (1, 0, 2)), validity)
    return jnp.transpose(filled, (1, 0, 2))


def solution(mesh):
    torus = Mesh(
        mesh.devices.reshape(4, 4, mesh.shape["pix"], mesh.shape["tile"]),
        ("date_0", "date_1", "pix", "tile"),
    )
    placed = (P(DATE, None, ("tile", "pix")), P(DATE, ("tile", "pix")), P(DATE))
    return jax.shard_map(
        body, mesh=torus, in_specs=placed, out_specs=P(DATE, None, ("tile", "pix")), check_vma=False
    )
```

```python
import functools

import jax
import jax.numpy as jnp
from jax import lax
from jax.experimental import pallas as pl
from jax.experimental.pallas import tpu as pltpu
from jax.sharding import Mesh
from jax.sharding import PartitionSpec as P

MESH = pl.DeviceIdType.MESH
DATE = ("date_0", "date_1")
LANES = 128
ROWS = 8
TILES = 4
FAR_FIRST = (1, 0, 2)
SIDE = 4
NONE = -1073741824.0
STRAIGHT, TURNED = 1, 2
SHARES = (-1, 1, 2, 2, 2, 2, 1, -1, -1)
LOADS = (2, 14)
UNIT, HOP, FAR = 0.35, 3.0, 4.0
EARLY, MIDDLE = 5, 11
TURN = 16


def pieces(shares, groups):
    if sum(abs(s) for s in shares) != groups:
        return [(g, 1) for g in range(groups)]
    starts, at = [], 0
    for share in shares:
        starts.append((at, abs(share)))
        at += abs(share)
    return starts


def plan(groups):
    across, turned = (STRAIGHT, TURNED) if groups > STRAIGHT + TURNED else (1, 1)
    hyper = groups - across - turned
    parts = pieces(SHARES, hyper)
    split = [s < 0 for s in SHARES] if len(parts) == len(SHARES) else [False] * len(parts)
    messages, owner = [], []
    for r, (start, count) in enumerate(parts):
        for side in (0, 1) if split[r] else (None,):
            messages.append((start, count, side or 0, 2 if side is None else 1))
            owner.append(r)
    rows = [*parts, (hyper, across), (hyper + across, turned)]
    load = 2 * across * UNIT
    events, first, second = [], 0.0, 2 * load
    ready, straight = [], 0.0
    for i, m in enumerate(messages):
        if i == min(EARLY, len(messages) - 1):
            first += load
        if i == min(MIDDLE, len(messages) - 1):
            first += load
            straight = first + HOP
        first += m[1] * m[3] * UNIT
        ready.append(first + HOP)
        events.append((ready[i], 0, i))
    events.append((straight, 2, 0))
    done = [0.0] * (len(rows) - 1)
    done[-1] = straight
    for i, m in enumerate(messages):
        second = max(second, ready[i]) + m[1] * m[3] * UNIT
        events.append((second + HOP, 1, i))
        done[owner[i]] = second + HOP
    link = 0.0
    for r in sorted(range(len(done)), key=lambda r: done[r]):
        link = max(link, done[r]) + 2 * UNIT * rows[r][1]
        events.append((link + FAR, 3, r))
    events.append((TURN, 4, 0))
    events.append((max(TURN, first, second) + 4 * turned * UNIT + FAR, 5, 0))
    return messages, owner, rows, [(kind, i) for _, kind, i in sorted(events)]


def scan_fill(
    bands,
    groups,
    days_hbm,
    x_hbm,
    v_hbm,
    out_ref,
    days,
    xv,
    vv,
    own,
    come,
    come_x,
    come_y,
    enter,
    day_sem,
    x_sem,
    v_sem,
    send_sem,
    recv_sem,
):
    width = TILES * LANES
    packs = (bands + 1) // 2
    loads = pieces(LOADS, groups)
    messages, owner, row_parts, order = plan(groups)
    straight, turned = row_parts[-2:]
    places = (pl.ds(0, straight[1]), pl.ds(straight[1], turned[1]))
    yi = lax.axis_index(DATE[0])
    xi = lax.axis_index(DATE[1])
    pair = ({DATE[1]: xi + 1 - 2 * lax.rem(xi, 2)}, {DATE[1]: 3 - xi})
    taken = (1 - lax.rem(xi, 2), 1 - xi // 2)
    rows = [{DATE[0]: lax.rem(yi + d, SIDE)} for d in range(1, SIDE)]
    row_gives = [(yi + d) // SIDE for d in range(1, SIDE)]
    row_takes = [1 - (yi + SIDE - d) // SIDE for d in range(1, SIDE)]
    crossing = (pair[1], {DATE[1]: lax.rem(xi + 2, SIDE)}, pair[0])
    cross_takes = (1 - xi // 2, 1 - xi // 2, 1 - lax.rem(xi, 2))

    def load_x(i):
        cols = pl.ds(loads[i][0] * width, loads[i][1] * width)
        return pltpu.make_async_copy(x_hbm.at[:, :, cols], xv.at[:, :, cols], x_sem.at[i])

    def load_v(i):
        cols = pl.ds(loads[i][0] * width, loads[i][1] * width)
        return pltpu.make_async_copy(v_hbm.at[:, cols], vv.at[:, cols], v_sem.at[i])

    def swap(stage, m):
        start, count, side, sides = messages[m]
        part, which = pl.ds(start, count), pl.ds(side, sides)
        return pltpu.make_async_remote_copy(
            src_ref=own.at[stage, part, which],
            dst_ref=come.at[stage, part, which],
            send_sem=send_sem.at[stage],
            recv_sem=recv_sem.at[stage * len(messages) + m],
            device_id=pair[stage],
            device_id_type=MESH,
        )

    def cross(turn, i):
        return pltpu.make_async_remote_copy(
            src_ref=own.at[1 + cross_takes[i], pl.ds(*turned)] if turn else own.at[0, pl.ds(*straight)],
            dst_ref=come_x.at[i, places[turn]],
            send_sem=send_sem.at[2],
            recv_sem=recv_sem.at[2 * len(messages) + turn],
            device_id=crossing[i],
            device_id_type=MESH,
        )

    def crossed(part, turn):
        return pltpu.make_async_remote_copy(
            src_ref=part,
            dst_ref=part,
            send_sem=send_sem.at[2],
            recv_sem=recv_sem.at[2 * len(messages) + turn],
            device_id=crossing[0],
            device_id_type=MESH,
        )

    def row_sem(r):
        return recv_sem.at[2 * len(messages) + 2 + r]

    def to_row(d, r):
        part = pl.ds(*row_parts[r])
        return pltpu.make_async_remote_copy(
            src_ref=own.at[0 if r == len(row_parts) - 1 else 2, part, row_gives[d]],
            dst_ref=come_y.at[part, d],
            send_sem=send_sem.at[3],
            recv_sem=row_sem(r),
            device_id=rows[d],
            device_id_type=MESH,
        )

    def from_rows(part, r):
        return pltpu.make_async_remote_copy(
            src_ref=come_y.at[part],
            dst_ref=come_y.at[part],
            send_sem=send_sem.at[3],
            recv_sem=row_sem(r),
            device_id=rows[0],
            device_id_type=MESH,
        )

    barrier = pltpu.get_barrier_semaphore()
    for who in (*crossing, *rows):
        pl.semaphore_signal(barrier, inc=1, device_id=who, device_id_type=MESH)
    day_copy = pltpu.make_async_copy(days_hbm, days, day_sem)
    day_copy.start()
    for i in range(len(loads)):
        load_v(i).start()
        load_x(i).start()

    day_copy.wait()
    sub = lax.broadcasted_iota(jnp.int32, (ROWS, LANES), 0)
    day_col = jnp.zeros((ROWS, LANES), jnp.float32)
    for t in range(ROWS):
        day_col = jnp.where(sub == t, days[t].astype(jnp.float32), day_col)
    key_rows = sub >= TILES

    def lanes_of(g, j):
        return pl.ds(pl.multiple_of(g * width + j * LANES, LANES), LANES)

    def key_of(pack):
        return jnp.where(key_rows, pack, pltpu.roll(pack, TILES, axis=0))

    def spread(row):
        return jnp.broadcast_to(row, (ROWS, LANES))

    def row_of(band, j):
        return band // 2, pl.ds((band % 2) * TILES + j, 1)

    def over(start, count, work):
        if count == 1:
            work(start)
        else:
            pl.loop(start, start + count)(work)

    def summarize(g):
        for j in range(TILES):
            cols = lanes_of(g, j)
            live = vv[:, cols] > 0
            last = jnp.max(jnp.where(live, day_col, NONE), axis=0, keepdims=True)
            first = jnp.max(jnp.where(live, -day_col, NONE), axis=0, keepdims=True)
            at_last = day_col == spread(last)
            at_first = -day_col == spread(first)
            for b in range(bands):
                x = xv[b, :, cols]
                p, r = row_of(b, j)
                own[0, g, 0, p, r, :] = jnp.sum(jnp.where(at_last, x, 0.0), axis=0, keepdims=True)
                own[0, g, 1, p, r, :] = jnp.sum(jnp.where(at_first, x, 0.0), axis=0, keepdims=True)
            p, r = row_of(bands, j)
            own[0, g, 0, p, r, :] = last
            own[0, g, 1, p, r, :] = first

    def merge_pair(stage, sides, g):
        for side in sides:
            take = key_of(come[stage, g, side, packs - 1]) > key_of(own[stage, g, side, packs - 1])
            for p in range(packs):
                own[stage + 1, g, side, p] = jnp.where(
                    take, come[stage, g, side, p], own[stage, g, side, p]
                )

    def enter_less(g, side, packs_of):
        take = key_of(packs_of(packs - 1)) > key_of(enter[g, side, packs - 1])
        for p in range(packs):
            enter[g, side, p] = jnp.where(take, packs_of(p), enter[g, side, p])

    def clear(g, side):
        for p in range(packs):
            enter[g, side, p] = jnp.where(key_rows, NONE if p == packs - 1 else 0.0, 0.0)

    def note_pair(g):
        side = taken[0]
        clear(g, 1 - side)
        for p in range(packs):
            enter[g, side, p] = come[0, g, side, p]
        enter_less(g, taken[1], lambda p: come[1, g, taken[1], p])

    def merge_cross(k):
        g = straight[0] + k
        for side in range(2):
            best = [own[0, g, side, p] for p in range(packs)]
            for i in range(SIDE - 1):
                take = key_of(come_x[i, k, side, packs - 1]) > key_of(best[-1])
                best = [jnp.where(take, come_x[i, k, side, p], best[p]) for p in range(packs)]
            for p in range(packs):
                own[2, g, side, p] = best[p]

    def note_cross(k):
        g = straight[0] + k
        for side in range(2):
            clear(g, side)
        for i in range(SIDE - 1):
            enter_less(g, cross_takes[i], lambda p: come_x[i, k, cross_takes[i], p])

    def note_rows(g):
        for d in range(SIDE - 1):
            enter_less(g, row_takes[d], lambda p: come_y[g, d, p])

    def turn_along(k):
        g = turned[0] + k
        for side in range(2):
            clear(g, side)
        note_rows(g)
        for side in range(2):
            take = key_of(own[0, g, side, packs - 1]) > key_of(enter[g, side, packs - 1])
            for p in range(packs):
                before = enter[g, side, p]
                own[2 - side, g, side, p] = jnp.where(take, own[0, g, side, p], before)
                own[1 + side, g, side, p] = before

    def complete_rows(g):
        note_rows(g)
        complete(g)

    def complete_turned(k):
        g = turned[0] + k
        for i in range(SIDE - 1):
            for side in range(2):
                enter_less(g, side, lambda p: come_x[i, straight[1] + k, side, p])
        complete(g)

    def complete(g):
        has = [key_of(enter[g, s, packs - 1]) > NONE for s in range(2)]
        mine = [key_of(own[0, g, s, packs - 1]) > NONE for s in range(2)]
        for p in range(packs):
            ends = [enter[g, s, p] for s in range(2)]
            other = [jnp.where(mine[s], own[0, g, s, p], ends[s]) for s in range(2)]
            if p == packs - 1:
                other = [jnp.where(key_rows, -o, o) for o in other]
            for s in range(2):
                enter[g, s, p] = jnp.where(has[s], ends[s], other[1 - s])
        for j in range(TILES):
            cols = lanes_of(g, j)
            live = vv[:, cols] > 0
            before = jnp.where(live, sub, -1)
            after = jnp.where(live, sub, ROWS)
            for k in (1, 2, 4):
                before = jnp.maximum(
                    before, jnp.where(sub >= k, pltpu.roll(before, k, axis=0), -1)
                )
                after = jnp.minimum(
                    after, jnp.where(sub < ROWS - k, pltpu.roll(after, ROWS - k, axis=0), ROWS)
                )
            has_f = before >= 0
            has_b = after < ROWS
            at_f = jnp.maximum(before, 0)
            at_b = jnp.minimum(after, ROWS - 1)

            def sides(x, b, sign):
                p, r = row_of(b, j)
                f = jnp.take_along_axis(x, at_f, axis=0)
                n = jnp.take_along_axis(x, at_b, axis=0)
                f = jnp.where(has_f, f, spread(enter[g, 0, p, r, :]))
                n = jnp.where(has_b, n, spread(sign * enter[g, 1, p, r, :]))
                return f, n

            prev, following = sides(day_col, bands, -1.0)
            span = following - prev
            weight = (day_col - prev) / jnp.where(span == 0.0, 1.0, span)
            for b in range(bands):
                f, n = sides(xv[b, :, cols], b, 1.0)
                out_ref[b, :, cols] = f + weight * (n - f)

    loaded = 0

    def summarize_part(start, count):
        nonlocal loaded
        while loaded < len(loads) and loads[loaded][0] < start + count:
            load_v(loaded).wait()
            load_x(loaded).wait()
            loaded += 1
        over(start, count, summarize)

    summarized = set()
    for m, (start, count, _, _) in enumerate(messages):
        if m == min(MIDDLE, len(messages) - 1):
            cross(0, 2).start()
        if start not in summarized:
            summarize_part(start, count)
            summarized.add(start)
        if m == 0:
            pl.semaphore_wait(barrier, len(pair) + len(rows) + 1)
        swap(0, m).start()
        if m == min(EARLY, len(messages) - 1) - 1 or len(messages) == 1:
            summarize_part(*turned)
            for d in range(SIDE - 1):
                to_row(d, len(row_parts) - 1).start()
            summarize_part(*straight)
            cross(0, 0).start()
            cross(0, 1).start()

    for kind, i in order:
        if kind < 2:
            start, count, side, sides = messages[i]
            swap(kind, i).wait_recv()
            over(start, count, functools.partial(merge_pair, kind, range(side, side + sides)))
            if kind == 0:
                swap(1, i).start()
            else:
                for d in FAR_FIRST:
                    if sides == 2:
                        to_row(d, owner[i]).start()
                    else:
                        pl.when(row_gives[d] == side)(to_row(d, owner[i]).start)
                if side + sides == 2:
                    over(start, count, note_pair)
        elif kind == 2:
            crossed(come_x.at[:, places[0]], 0).wait_recv()
            over(0, straight[1], merge_cross)
            for d in FAR_FIRST:
                to_row(d, len(row_parts) - 2).start()
            over(0, straight[1], note_cross)
        elif kind == 3:
            from_rows(pl.ds(*row_parts[i]), i).wait_recv()
            over(*row_parts[i], complete_rows)
        elif kind == 4:
            from_rows(pl.ds(*turned), len(row_parts) - 1).wait_recv()
            over(0, turned[1], turn_along)
            for k in range(SIDE - 1):
                cross(1, k).start()
        else:
            crossed(come_x.at[:, places[1]], 1).wait_recv()
            over(0, turned[1], complete_turned)

    for stage in range(2):
        part = pl.ds(0, straight[0])
        pltpu.make_async_remote_copy(
            src_ref=own.at[stage, part],
            dst_ref=come.at[stage, part],
            send_sem=send_sem.at[stage],
            recv_sem=recv_sem.at[0],
            device_id=pair[stage],
            device_id_type=MESH,
        ).wait_send()
    crossed(come_x, 0).wait_send()
    from_rows(pl.ds(0, groups), 0).wait_send()


def body(reflectance, validity, day_number):
    dates, bands, pixels = reflectance.shape
    groups = pixels // (TILES * LANES)
    packs = (bands + 1) // 2
    messages, _, rows, _ = plan(groups)
    loads = len(pieces(LOADS, groups))
    hbm = pl.BlockSpec(memory_space=pltpu.HBM)
    filled = pl.pallas_call(
        functools.partial(scan_fill, bands, groups),
        out_shape=pltpu.VMEM((bands, dates, pixels), jnp.float32),
        in_specs=[hbm, hbm, hbm],
        out_specs=pl.BlockSpec(memory_space=pltpu.VMEM),
        scratch_shapes=[
            pltpu.SMEM((dates,), jnp.int32),
            pltpu.VMEM((bands, dates, pixels), jnp.float32),
            pltpu.VMEM((dates, pixels), jnp.int32),
            pltpu.VMEM((3, groups, 2, packs, ROWS, LANES), jnp.float32),
            pltpu.VMEM((2, groups, 2, packs, ROWS, LANES), jnp.float32),
            pltpu.VMEM((SIDE - 1, rows[-2][1] + rows[-1][1], 2, packs, ROWS, LANES), jnp.float32),
            pltpu.VMEM((groups, SIDE - 1, packs, ROWS, LANES), jnp.float32),
            pltpu.VMEM((groups, 2, packs, ROWS, LANES), jnp.float32),
            pltpu.SemaphoreType.DMA,
            pltpu.SemaphoreType.DMA((loads,)),
            pltpu.SemaphoreType.DMA((loads,)),
            pltpu.SemaphoreType.DMA((4,)),
            pltpu.SemaphoreType.DMA((2 * len(messages) + 2 + len(rows),)),
        ],
        compiler_params=pltpu.CompilerParams(
            collective_id=0, has_side_effects=True, vmem_limit_bytes=(62 << 20) - 65536
        ),
        name="scan_fill",
    )(day_number, jnp.transpose(reflectance, (1, 0, 2)), validity)
    return jnp.transpose(filled, (1, 0, 2))


def solution(mesh):
    torus = Mesh(
        mesh.devices.reshape(4, 4, mesh.shape["pix"], mesh.shape["tile"]),
        ("date_0", "date_1", "pix", "tile"),
    )
    placed = (P(DATE, None, ("tile", "pix")), P(DATE, ("tile", "pix")), P(DATE))
    return jax.shard_map(
        body, mesh=torus, in_specs=placed, out_specs=P(DATE, None, ("tile", "pix")), check_vma=False
    )
```
